256 devices in a mesh: req: 8 (over x, core), seq: 32 (over y, z).
Axes of the slice: x: 4, y: 4, z: 8, core: 2. Of those that a mesh axis runs over, the one named last changes fastest.
Arguments:
- query_nope: bfloat16 [16, 2, 128, 128], P('req', None, 'seq'), may hold values from -12 to 12
- query_rope: bfloat16 [16, 2, 8192], P('req', None, 'seq'), may hold values from -32 to 32
- key_absorb: bfloat16 [128, 128, 512], P('seq'), may hold values from -0.5 to 0.5
- value_up_matrix: bfloat16 [128, 512, 128], P('seq'), may hold values from -0.5 to 0.5
- latent_cache: bfloat16 [16, 131072, 512], P('req', 'seq'), may hold values from -6 to 6
- rope_cache: bfloat16 [16, 64, 131072], P('req', None, 'seq'), may hold values from -4 to 4
- new_latent: bfloat16 [16, 2, 512], P('req'), may hold values from -12 to 12
- new_rope: bfloat16 [16, 2, 64], P('req'), may hold values from -10 to 10
- lengths: int32 [16], P('req'), may hold values from 1 to 131072
- positions: int32 [16, 2], P('req'), may hold values from 0 to 8191
Outputs:
- head_outputs: bfloat16 [16, 2, 128, 128], P('req', None, 'seq')
The draws below stay inside these ranges and needn't reach their ends.
All inputs are finite; a program needn't handle non-finite values.
Results may differ from the reference program's by a relative error of at most 0.0087.
Values may be sent and summed in bfloat16 or wider, within the bound.
A program may use at most 64 MiB of HBM per device.

```python
import jax
import jax.numpy as jnp
from jax import lax

H = 128
KVL = 512
ROPE = 64
NOPE = 128
VH = 128
STEPS = 2
REQUESTS = 16
CTX = 131072


def rope_pair(key):
    query_start_offset = jnp.clip(jax.random.normal(jax.random.fold_in(key, 101), (REQUESTS, STEPS, H, ROPE), jnp.float32), -4.0, 4.0)
    key_start_offset = jnp.clip(jax.random.normal(jax.random.fold_in(key, 102), (REQUESTS, ROPE, CTX), jnp.float32), -4.0, 4.0)
    return (query_start_offset.reshape(REQUESTS, STEPS, H * ROPE), key_start_offset)


def draw_query_rope(key, part):
    return rope_pair(key)[0].astype(jnp.bfloat16)


def draw_rope_cache(key, part):
    return rope_pair(key)[1].astype(jnp.bfloat16)


def set_ends(drawn, rng, low, largest):
    longest = drawn.shape.index(max(drawn.shape))
    spots = []
    for shift in (0, 1):
        where = [jax.random.randint(jax.random.fold_in(rng, axis), (), 0, length) for axis, length in enumerate(drawn.shape)]
        where[longest] = (where[longest] + shift) % drawn.shape[longest]
        spots.append(tuple(where))
    return drawn.at[spots[0]].set(low).at[spots[1]].set(largest)


def level_of(rng, dims, cuts, least, largest):
    factor_of, own = 1.0, jax.random.fold_in(rng, 6)
    for position, shards_of in cuts:
        steps = jnp.exp(jax.random.uniform(jax.random.fold_in(own, position), (shards_of,), jnp.float32, least / len(cuts), largest / len(cuts)))
        factor_of = factor_of * jnp.repeat(steps, dims[position] // shards_of).reshape([-1 if axis == position else 1 for axis in range(len(dims))])
    return factor_of


def noise(own_key, dims, spread, bound, split=(), kind=jnp.bfloat16):
    entries = jax.random.normal(own_key, dims, jnp.float32) * spread
    if len(split) > 0:
        entries = level_of(own_key, dims, split, -0.22, 0.18) * entries
    return jnp.clip(entries, min=-bound, max=bound).astype(kind)


def setup_inputs(seed: int = 0) -> dict:
    streams_of = jax.random.split(jax.random.key(seed), 11)
    query_nope = noise(streams_of[0], (REQUESTS, STEPS, H, NOPE), 2.0, 12.0, ((0, 8), (2, 32)))
    query_rope = draw_query_rope(jax.random.fold_in(streams_of[10], 71), 0)
    key_absorb = noise(streams_of[2], (H, NOPE, KVL), NOPE ** -0.5, 0.5, ((0, 32),))
    value_up_matrix = noise(streams_of[3], (H, KVL, VH), (KVL // 4) ** -0.5, 0.5, ((0, 32),))
    latent_cache = noise(streams_of[4], (REQUESTS, CTX, KVL), 1.0, 6.0, ((0, 8), (1, 32)))
    rope_cache = draw_rope_cache(jax.random.fold_in(streams_of[10], 71), 0)
    new_latent = noise(streams_of[6], (REQUESTS, STEPS, KVL), 2.5, 12.0, ((0, 8),))
    new_rope = noise(streams_of[7], (REQUESTS, STEPS, ROPE), 2.0, 10.0, ((0, 8),))
    lengths = set_ends(jax.random.randint(streams_of[8], (REQUESTS,), 1, CTX + 1), jax.random.fold_in(streams_of[8], 1), 1, CTX).astype(jnp.int32)
    positions = set_ends(jax.random.randint(streams_of[9], (REQUESTS, STEPS), 0, 8192), jax.random.fold_in(streams_of[9], 1), 0, 8191).astype(jnp.int32)
    return dict(query_nope=query_nope, query_rope=query_rope, key_absorb=key_absorb, value_up_matrix=value_up_matrix, latent_cache=latent_cache, rope_cache=rope_cache, new_latent=new_latent, new_rope=new_rope, lengths=lengths, positions=positions)


NEG_FILL = -1e30


def rotate(vectors, where_at):
    half_width = vectors.shape[-1] // 2
    frequency = 10000.0 ** (-jnp.arange(half_width, dtype=jnp.float32) / half_width)
    angles = where_at.astype(jnp.float32)[..., None] * frequency
    leading = vectors[..., :half_width].astype(jnp.float32)
    trailing = vectors[..., half_width:].astype(jnp.float32)
    return jnp.concatenate([leading * jnp.cos(angles) - trailing * jnp.sin(angles), leading * jnp.sin(angles) + trailing * jnp.cos(angles)], axis=-1)


def reference(query_nope, query_rope, key_absorb, value_up_matrix, latent_cache, rope_cache, new_latent, new_rope, lengths, positions):
    softmax_scale = (NOPE + ROPE) ** -0.5
    query_latent = jnp.einsum('rshn,hnk->rshk', query_nope.astype(jnp.float32), key_absorb.astype(jnp.float32)).astype(jnp.bfloat16)
    query_rotary = query_rope.reshape(REQUESTS, STEPS, H, ROPE)
    key_new = rotate(new_rope, positions).astype(jnp.bfloat16)
    causal = jnp.arange(STEPS)[None, :] <= jnp.arange(STEPS)[:, None]

    def one_request(items):
        latent_query, rotary_query, cached, rotary_cached, latent_new, rotary_new, length = items
        is_valid_entry = jnp.arange(CTX) < length
        cache_score = (jnp.einsum('shk,tk->sht', latent_query.astype(jnp.float32), cached.astype(jnp.float32)) + jnp.einsum('shd,dt->sht', rotary_query.astype(jnp.float32), rotary_cached.astype(jnp.float32))) * softmax_scale
        cache_score = jnp.where(is_valid_entry[None, None, :], cache_score, NEG_FILL)
        new_score = (jnp.einsum('shk,jk->shj', latent_query.astype(jnp.float32), latent_new.astype(jnp.float32)) + jnp.einsum('shd,jd->shj', rotary_query.astype(jnp.float32), rotary_new.astype(jnp.float32))) * softmax_scale
        new_score = jnp.where(causal[:, None, :], new_score, NEG_FILL)
        highest = jnp.maximum(jnp.max(cache_score, axis=-1), jnp.max(new_score, axis=-1))
        cache_weight = jnp.where(is_valid_entry[None, None, :], jnp.exp(cache_score - highest[..., None]), 0.0)
        new_weight = jnp.where(causal[:, None, :], jnp.exp(new_score - highest[..., None]), 0.0)
        total = jnp.sum(cache_weight, axis=-1) + jnp.sum(new_weight, axis=-1)
        mixed = jnp.einsum('sht,tk->shk', cache_weight.astype(jnp.bfloat16).astype(jnp.float32), cached.astype(jnp.float32))
        mixed = mixed + jnp.einsum('shj,jk->shk', new_weight.astype(jnp.bfloat16).astype(jnp.float32), latent_new.astype(jnp.float32))
        return (mixed / total[..., None]).astype(jnp.bfloat16)

    latent_result = lax.map(one_request, (query_latent, query_rotary, latent_cache, rope_cache, new_latent, key_new, lengths))
    return jnp.einsum('ufia,iaj->ufij', latent_result.astype(jnp.float32), value_up_matrix.astype(jnp.float32)).astype(jnp.bfloat16)
```

```python
import functools

import jax
import jax.numpy as jnp
import numpy as np
from jax import lax
from jax.experimental import pallas as pl
from jax.experimental.pallas import tpu as pltpu
from jax.sharding import PartitionSpec as P

F32 = jnp.float32
BF16 = jnp.bfloat16
MASKED = -1e30
FLOOR = -1e29
NY, NZ = 4, 8
SHARDS = NY * NZ
REQS, STEPS, HEADS, NOPE, KVL, ROPE, VH = 2, 2, 4, 128, 512, 64, 128
ROWS = STEPS * HEADS
ALL = SHARDS * ROWS
KEYS = 4096
WIDE = KVL + 128
SCORE_SCALE = float((NOPE + ROPE) ** -0.5 * np.log2(np.e))
NT = (((1,), (1,)), ((), ()))
CHUNK1, SUB1 = 2048, 512
CHUNK2, SUB2 = 2048, 256
FAR_Z = (4, 3, 5, 2, 6, 1, 7)
FAR_Y = (2, 1, 3)


def iota(shape, dim):
    return lax.broadcasted_iota(jnp.int32, shape, dim)


def rounded(x):
    return x.astype(BF16).astype(F32)


def encode(maxima, totals):
    rows = maxima.shape[0]
    lane = iota((rows, 128), 1)
    high = rounded(maxima)
    middle = rounded(maxima - high)
    low = maxima - high - middle
    total_high = rounded(totals)
    total_low = totals - total_high
    tile = jnp.where(lane == 0, high, 0.0)
    tile = jnp.where(lane == 1, middle, tile)
    tile = jnp.where(lane == 2, low, tile)
    tile = jnp.where(lane == 3, total_high, tile)
    return jnp.where(lane == 4, total_low, tile)


def decode(tile):
    lane = iota(tile.shape, 1)
    maxima = jnp.sum(jnp.where(lane < 3, tile, 0.0), axis=1, keepdims=True)
    totals = jnp.sum(jnp.where(lane < 3, 0.0, tile), axis=1, keepdims=True)
    return maxima, totals


def merge(parts):
    highest = functools.reduce(jnp.maximum, [m for _, m, _ in parts])
    sums, totals = 0.0, 0.0
    for s, m, t in parts:
        factor = jnp.exp2(m - highest)
        sums = sums + s * factor
        totals = totals + t * factor
    return sums, highest, totals


def unpack(block):
    wide = block.astype(F32)
    return (wide[:, :KVL],) + decode(wide[:, KVL:])


def kernel(
    nope_ref, rope_ref, absorb_hbm, value_hbm, latent_hbm, keys_hbm,
    new_latent_ref, new_rope_ref, freq_ref, lengths_ref, positions_ref,
    out_ref,
    absorb, value, latent, keys, qa, qb, qfull, scores, acc, local_q,
    partial, yrecv, zsend, zrecv,
    load_sem, agz_s, agz_r, agy_s, agy_r, rsy_s, rsy_r, rsz_s, rsz_r,
):
    seq = lax.axis_index("seq")
    y = seq // NZ
    z = seq % NZ

    def at_z(d):
        return {"seq": y * NZ + (z + d) % NZ}

    def at_y(d):
        return {"seq": ((y + d) % NY) * NZ + z}

    barrier = pltpu.get_barrier_semaphore()
    for d in FAR_Z:
        pl.semaphore_signal(barrier, inc=1, device_id=at_z(d), device_id_type=pl.DeviceIdType.MESH)
    for d in FAR_Y:
        pl.semaphore_signal(barrier, inc=1, device_id=at_y(d), device_id_type=pl.DeviceIdType.MESH)

    loads = [
        pltpu.make_async_copy(absorb_hbm, absorb, load_sem.at[0]),
        pltpu.make_async_copy(latent_hbm.at[0], latent.at[0], load_sem.at[1]),
        pltpu.make_async_copy(keys_hbm, keys, load_sem.at[2]),
        pltpu.make_async_copy(latent_hbm.at[1], latent.at[1], load_sem.at[3]),
        pltpu.make_async_copy(value_hbm, value, load_sem.at[4]),
    ]
    for copy in loads:
        copy.start()

    rope_q = rope_ref[...].astype(F32)
    row8 = iota((ROWS, HEADS * ROPE), 0)
    lane256 = iota((ROWS, HEADS * ROPE), 1)
    fold_row = iota((HEADS * ROPE, 128), 0)
    fold_lane = iota((HEADS * ROPE, 128), 1)
    rope_tile = jnp.zeros((ROWS, 128), F32)
    for r in range(REQS):
        spread = jnp.where(row8 < HEADS, rope_q[r, 0:1], rope_q[r, 1:2])
        spread = jnp.where(lane256 // ROPE == row8 % HEADS, spread, 0.0).astype(BF16)
        fold = jnp.where(fold_row % ROPE + r * ROPE == fold_lane, 1.0, 0.0).astype(BF16)
        rope_tile = rope_tile + jnp.dot(spread, fold, preferred_element_type=F32)
    nope_q = nope_ref[...].astype(F32)
    row16 = iota((REQS * ROWS, NOPE), 0)
    spread = [jnp.where(row16 % HEADS == h, nope_q, 0.0) for h in range(HEADS)]
    spread = jnp.concatenate(spread, axis=1).astype(BF16)
    loads[0].wait()
    lat_q = jnp.dot(spread, absorb[...], preferred_element_type=F32).astype(BF16)
    local_q[...] = lat_q.astype(F32)
    lat_q = local_q[...]
    qa[seq, :, :KVL] = lat_q[:ROWS].astype(BF16)
    qa[seq, :, KVL:] = rope_tile.astype(BF16)
    qb[seq] = lat_q[ROWS:].astype(BF16)

    pl.semaphore_wait(barrier, NZ - 1 + NY - 1)

    queries = (qa, qb)

    def gather_z(r, d):
        mine = queries[r].at[seq]
        return pltpu.make_async_remote_copy(
            src_ref=mine, dst_ref=mine, send_sem=agz_s.at[r, d - 1], recv_sem=agz_r.at[r, d - 1],
            device_id=at_z(d), device_id_type=pl.DeviceIdType.MESH)

    def gather_y(r, d):
        mine = queries[r].at[pl.ds(y * NZ, NZ)]
        return pltpu.make_async_remote_copy(
            src_ref=mine, dst_ref=mine, send_sem=agy_s.at[r, d - 1], recv_sem=agy_r.at[r, d - 1],
            device_id=at_y(d), device_id_type=pl.DeviceIdType.MESH)

    def scatter_y(r, d):
        return pltpu.make_async_remote_copy(
            src_ref=partial.at[r, pl.ds(((y + d) % NY) * NZ, NZ)], dst_ref=yrecv.at[r, d - 1],
            send_sem=rsy_s.at[r, d - 1], recv_sem=rsy_r.at[r, d - 1],
            device_id=at_y(d), device_id_type=pl.DeviceIdType.MESH)

    def scatter_z(r, d):
        return pltpu.make_async_remote_copy(
            src_ref=zsend.at[r, (z + d) % NZ], dst_ref=zrecv.at[r, d - 1],
            send_sem=rsz_s.at[r, d - 1], recv_sem=rsz_r.at[r, d - 1],
            device_id=at_z(d), device_id_type=pl.DeviceIdType.MESH)

    for r in range(REQS):
        for d in FAR_Z:
            gather_z(r, d).start()

    freq = freq_ref[0:1]
    turn_sign = freq_ref[1:2]
    half_row = iota((ROPE, 128), 0)
    half_lane = iota((ROPE, 128), 1)
    new_latent = new_latent_ref[...].astype(F32)
    fresh = []
    lane_row = iota((8, 128), 0)
    positions = jnp.zeros((8, 128), jnp.int32)
    for r in range(REQS):
        for j in range(STEPS):
            positions = jnp.where(lane_row == r * STEPS + j, positions_ref[r, j], positions)
    angle = positions.astype(F32) * freq
    cosine, sine = jnp.cos(angle), jnp.sin(angle)
    row8n = iota((ROWS, 1), 0)
    for r in range(REQS):
        place = jnp.where(half_row + r * ROPE == half_lane, 1.0, 0.0).astype(BF16)
        swapped = jnp.where(
            (half_row + ROPE // 2) % ROPE + r * ROPE == half_lane, 1.0, 0.0).astype(BF16)
        plain = jnp.dot(new_rope_ref[...], place, preferred_element_type=F32)
        turned = jnp.dot(new_rope_ref[...], swapped, preferred_element_type=F32)
        found = []
        for j in range(STEPS):
            i = r * STEPS + j
            key = plain[i : i + 1] * cosine[i : i + 1] + turned[i : i + 1] * (sine[i : i + 1] * turn_sign)
            key = rounded(key)
            score = jnp.sum(lat_q[r * ROWS : (r + 1) * ROWS] * new_latent[r, j : j + 1], axis=1, keepdims=True)
            score = score + jnp.sum(rope_tile * key, axis=1, keepdims=True)
            found.append(jnp.where(row8n >= j * HEADS, score * SCORE_SCALE, MASKED))
        highest = functools.reduce(jnp.maximum, found)
        sums, totals = 0.0, 0.0
        for j in range(STEPS):
            weight = jnp.exp2(found[j] - highest)
            totals = totals + weight
            sums = sums + rounded(weight) * new_latent[r, j : j + 1]
        fresh.append((sums, highest, totals))

    for r in range(REQS):
        for d in FAR_Z:
            gather_z(r, d).wait_recv()
        for d in FAR_Y:
            gather_y(r, d).start()

    lane128 = iota((ALL, 128), 1)
    for r in range(REQS):
        for d in FAR_Y:
            gather_y(r, d).wait_recv()
        qfull[r] = queries[r][:, :, :KVL].astype(F32).reshape(ALL, KVL).astype(BF16)
        if r == 0:
            rotary = qa[:, :, KVL:].astype(F32).reshape(ALL, 128)
            loads[1].wait()
            loads[2].wait()
        else:
            loads[3].wait()
        own_rotary = jnp.where(lane128 // ROPE == r, rotary, 0.0).astype(BF16)
        query = qfull[r]
        live = lengths_ref[r] - seq * KEYS

        def score_chunk(c, peak):
            for i in range(CHUNK1 // SUB1):
                at = pl.multiple_of(c * CHUNK1 + i * SUB1, SUB1)
                s = lax.dot_general(query, latent[r, pl.ds(at, SUB1), :], NT, preferred_element_type=F32)
                s = s + jnp.dot(own_rotary, keys[:, pl.ds(at, SUB1)], preferred_element_type=F32)
                bias = jnp.where(at + iota((1, SUB1), 1) < live, 0.0, MASKED)
                s = s * SCORE_SCALE + bias
                scores[:, pl.ds(at, SUB1)] = s
                for t in range(SUB1 // 128):
                    peak = jnp.maximum(peak, s[:, t * 128 : (t + 1) * 128])
            return peak

        peak = lax.fori_loop(0, KEYS // CHUNK1, score_chunk, jnp.full((ALL, 128), FLOOR, F32))
        highest = jnp.max(peak, axis=1, keepdims=True)
        acc[...] = jnp.zeros_like(acc)

        def weigh_chunk(c, lane_sums):
            mixed = None
            for i in range(CHUNK2 // SUB2):
                at = pl.multiple_of(c * CHUNK2 + i * SUB2, SUB2)
                p = jnp.exp2(scores[:, pl.ds(at, SUB2)] - highest)
                for t in range(SUB2 // 128):
                    lane_sums = lane_sums + p[:, t * 128 : (t + 1) * 128]
                piece = jnp.dot(p.astype(BF16), latent[r, pl.ds(at, SUB2), :], preferred_element_type=F32)
                mixed = piece if mixed is None else mixed + piece
            acc[...] += mixed
            return lane_sums

        lane_sums = lax.fori_loop(0, KEYS // CHUNK2, weigh_chunk, jnp.zeros((ALL, 128), F32))
        totals = jnp.sum(lane_sums, axis=1, keepdims=True)
        partial[r, :, :, :KVL] = acc[...].reshape(SHARDS, ROWS, KVL).astype(BF16)
        partial[r, :, :, KVL:] = encode(highest, totals).reshape(SHARDS, ROWS, 128).astype(BF16)
        for d in FAR_Y:
            scatter_y(r, d).start()

    for r in range(REQS):
        parts = [unpack(partial[r, pl.ds(y * NZ, NZ)].astype(F32).reshape(NZ * ROWS, WIDE))]
        for d in (1, 3, 2):
            scatter_y(r, d).wait_recv()
            parts.append(unpack(yrecv[r, d - 1].astype(F32).reshape(NZ * ROWS, WIDE)))
        sums, highest, totals = merge(parts)
        zsend[r, :, :, :KVL] = sums.reshape(NZ, ROWS, KVL).astype(BF16)
        zsend[r, :, :, KVL:] = encode(highest, totals).reshape(NZ, ROWS, 128).astype(BF16)
        for d in FAR_Z:
            scatter_z(r, d).start()

    loads[4].wait()
    results = []
    for r in range(REQS):
        parts = [fresh[r], unpack(zsend[r, z].astype(F32))]
        for d in FAR_Z[::-1]:
            scatter_z(r, d).wait_recv()
            parts.append(unpack(zrecv[r, d - 1].astype(F32)))
        sums, highest, totals = merge(parts)
        results.append(rounded(sums / totals))
    result = jnp.concatenate(results, axis=0)
    row16v = iota((REQS * ROWS, KVL), 0)
    spread = [jnp.where(row16v % HEADS == h, result, 0.0) for h in range(HEADS)]
    spread = jnp.concatenate(spread, axis=1).astype(BF16)
    out_ref[...] = jnp.dot(spread, value[...], preferred_element_type=F32).astype(BF16)

    for r in range(REQS):
        for d in FAR_Z:
            gather_z(r, d).wait_send()
            scatter_z(r, d).wait_send()
        for d in FAR_Y:
            gather_y(r, d).wait_send()
            scatter_y(r, d).wait_send()


def frequency_rows():
    half = ROPE // 2
    lanes = np.arange(128)
    freq = (10000.0 ** (-(np.arange(half, dtype=np.float64)) / half)).astype(np.float32)
    sign = np.where(lanes % ROPE < half, -1.0, 1.0).astype(np.float32)
    return np.stack([freq[lanes % half], sign])


def on_device(
    query_nope, query_rope, key_absorb, value_up_matrix, latent_cache, rope_cache,
    new_latent, new_rope, lengths, positions,
):
    vmem = pl.BlockSpec(memory_space=pltpu.VMEM)
    smem = pl.BlockSpec(memory_space=pltpu.SMEM)
    hbm = pl.BlockSpec(memory_space=pl.ANY)
    out = pl.pallas_call(
        kernel,
        name="latent_attention",
        out_shape=jax.ShapeDtypeStruct((REQS * ROWS, VH), BF16),
        in_specs=[vmem, vmem, hbm, hbm, hbm, hbm, vmem, vmem, vmem, smem, smem],
        out_specs=vmem,
        scratch_shapes=[
            pltpu.VMEM((HEADS * NOPE, KVL), BF16),
            pltpu.VMEM((HEADS * KVL, VH), BF16),
            pltpu.VMEM((REQS, KEYS, KVL), BF16),
            pltpu.VMEM((REQS * ROPE, KEYS), BF16),
            pltpu.VMEM((SHARDS, ROWS, WIDE), BF16),
            pltpu.VMEM((SHARDS, ROWS, KVL), BF16),
            pltpu.VMEM((REQS, ALL, KVL), BF16),
            pltpu.VMEM((ALL, KEYS), F32),
            pltpu.VMEM((ALL, KVL), F32),
            pltpu.VMEM((REQS * ROWS, KVL), F32),
            pltpu.VMEM((REQS, SHARDS, ROWS, WIDE), BF16),
            pltpu.VMEM((REQS, NY - 1, NZ, ROWS, WIDE), BF16),
            pltpu.VMEM((REQS, NZ, ROWS, WIDE), BF16),
            pltpu.VMEM((REQS, NZ - 1, ROWS, WIDE), BF16),
            pltpu.SemaphoreType.DMA((5,)),
            pltpu.SemaphoreType.DMA((REQS, NZ - 1)),
            pltpu.SemaphoreType.DMA((REQS, NZ - 1)),
            pltpu.SemaphoreType.DMA((REQS, NY - 1)),
            pltpu.SemaphoreType.DMA((REQS, NY - 1)),
            pltpu.SemaphoreType.DMA((REQS, NY - 1)),
            pltpu.SemaphoreType.DMA((REQS, NY - 1)),
            pltpu.SemaphoreType.DMA((REQS, NZ - 1)),
            pltpu.SemaphoreType.DMA((REQS, NZ - 1)),
        ],
        compiler_params=pltpu.CompilerParams(collective_id=0, has_side_effects=True),
    )(
        query_nope.reshape(REQS * ROWS, NOPE),
        query_rope,
        key_absorb.reshape(HEADS * NOPE, KVL),
        value_up_matrix.reshape(HEADS * KVL, VH),
        latent_cache,
        rope_cache.reshape(REQS * ROPE, KEYS),
        new_latent,
        new_rope.reshape(REQS * STEPS, ROPE),
        jnp.asarray(frequency_rows()),
        lengths,
        positions,
    )
    return out.reshape(REQS, STEPS, HEADS, VH)


def solution(mesh):
    return jax.shard_map(
        on_device,
        mesh=mesh,
        in_specs=(
            P("req", None, "seq", None),
            P("req", None, "seq"),
            P("seq", None, None),
            P("seq", None, None),
            P("req", "seq", None),
            P("req", None, "seq"),
            P("req", None, None),
            P("req", None, None),
            P("req"),
            P("req", None),
        ),
        out_specs=P("req", None, "seq", None),
        check_vma=False,
    )
```

```python
import functools

import jax
import jax.numpy as jnp
import numpy as np
from jax import lax
from jax.experimental import pallas as pl
from jax.experimental.pallas import tpu as pltpu
from jax.sharding import PartitionSpec as P

F32 = jnp.float32
BF16 = jnp.bfloat16
MASKED = -1e30
FLOOR = -1e29
NY, NZ = 4, 8
SHARDS = NY * NZ
REQS, STEPS, HEADS, NOPE, KVL, ROPE, VH = 2, 2, 4, 128, 512, 64, 128
ROWS = STEPS * HEADS
ALL = SHARDS * ROWS
KEYS = 4096
WIDE = KVL + 128
SCORE_SCALE = float((NOPE + ROPE) ** -0.5 * np.log2(np.e))
SUB1 = 512
SUB2 = 256
FAR_Z = (4, 3, 5, 2, 6, 1, 7)
NEAR_Z = (1, 7, 2, 6, 3, 5, 4)
FAR_Y = (1, 3, 2)
VMEM_LIMIT = 40 << 20
GROUPS = (2, 1, 3, 0)
GROUP = NZ * ROWS


def iota(shape, dim):
    return lax.broadcasted_iota(jnp.int32, shape, dim)


def rounded(x):
    return x.astype(BF16).astype(F32)


def encode(maxima, totals):
    rows = maxima.shape[0]
    lane = iota((rows, 128), 1)
    high = rounded(maxima)
    middle = rounded(maxima - high)
    low = maxima - high - middle
    total_high = rounded(totals)
    total_low = totals - total_high
    tile = jnp.where(lane == 0, high, 0.0)
    tile = jnp.where(lane == 1, middle, tile)
    tile = jnp.where(lane == 2, low, tile)
    tile = jnp.where(lane == 3, total_high, tile)
    return jnp.where(lane == 4, total_low, tile)


def decode(tile):
    lane = iota(tile.shape, 1)
    maxima = jnp.sum(jnp.where(lane < 3, tile, 0.0), axis=1, keepdims=True)
    totals = jnp.sum(jnp.where(lane < 3, 0.0, tile), axis=1, keepdims=True)
    return maxima, totals


def merge(parts):
    highest = functools.reduce(jnp.maximum, [m for _, m, _ in parts])
    sums, totals = 0.0, 0.0
    for s, m, t in parts:
        factor = jnp.exp2(m - highest)
        sums = sums + s * factor
        totals = totals + t * factor
    return sums, highest, totals


def unpack(block):
    wide = block.astype(F32)
    return (wide[:, :KVL],) + decode(wide[:, KVL:])


def unpack_y(block, stats):
    columns = stats.T
    return block.astype(F32).reshape(GROUP, KVL), columns[:, 0:1], columns[:, 1:2]


def kernel(
    nope_hbm, rope_hbm, absorb_hbm, value_hbm, latent_hbm, keys_hbm,
    new_latent_hbm, new_rope_hbm, freq_hbm, lengths_hbm, positions_hbm,
    out_ref,
    nope_ref, rope_ref, new_latent_ref, new_rope_ref, freq_ref, lengths_ref, positions_ref,
    absorb, value, latent, keys, qa, qb, qfull, rotary, flipped, scores, local_q,
    partial, stats, yrecv, ystats, zsend, zrecv,
    small_sem, load_sem, agz_s, agz_r, agy_s, agy_r, rsy_s, rsy_r, rst_s, rst_r, rsz_s, rsz_r,
):
    seq = lax.axis_index("seq")
    y = seq // NZ
    z = seq % NZ

    def at_z(d):
        return {"seq": y * NZ + (z + d) % NZ}

    def at_y(d):
        return {"seq": ((y + d) % NY) * NZ + z}

    barrier = pltpu.get_barrier_semaphore()
    for d in FAR_Z:
        pl.semaphore_signal(barrier, inc=1, device_id=at_z(d), device_id_type=pl.DeviceIdType.MESH)
    for d in FAR_Y:
        pl.semaphore_signal(barrier, inc=1, device_id=at_y(d), device_id_type=pl.DeviceIdType.MESH)

    small = (
        (nope_hbm, nope_ref), (rope_hbm, rope_ref), (new_latent_hbm, new_latent_ref),
        (new_rope_hbm, new_rope_ref), (freq_hbm, freq_ref), (lengths_hbm, lengths_ref),
        (positions_hbm, positions_ref),
    )
    small_loads = [pltpu.make_async_copy(a, b, small_sem.at[i]) for i, (a, b) in enumerate(small)]
    for copy in small_loads:
        copy.start()
    loads = [
        pltpu.make_async_copy(absorb_hbm, absorb, load_sem.at[0]),
        pltpu.make_async_copy(latent_hbm.at[0], latent.at[0], load_sem.at[1]),
        pltpu.make_async_copy(keys_hbm, keys, load_sem.at[2]),
        pltpu.make_async_copy(latent_hbm.at[1], latent.at[1], load_sem.at[3]),
        pltpu.make_async_copy(value_hbm, value, load_sem.at[4]),
    ]
    for copy in loads:
        copy.start()

    small_loads[1].wait()
    rope_q = rope_ref[...].astype(F32)
    row8 = iota((ROWS, HEADS * ROPE), 0)
    lane256 = iota((ROWS, HEADS * ROPE), 1)
    fold_row = iota((HEADS * ROPE, 128), 0)
    fold_lane = iota((HEADS * ROPE, 128), 1)
    rope_tile = jnp.zeros((ROWS, 128), F32)
    for r in range(REQS):
        spread = jnp.where(row8 < HEADS, rope_q[r, 0:1], rope_q[r, 1:2])
        spread = jnp.where(lane256 // ROPE == row8 % HEADS, spread, 0.0).astype(BF16)
        fold = jnp.where(fold_row % ROPE + r * ROPE == fold_lane, 1.0, 0.0).astype(BF16)
        rope_tile = rope_tile + jnp.dot(spread, fold, preferred_element_type=F32)
    small_loads[0].wait()
    nope_q = nope_ref[...].astype(F32)
    row16 = iota((REQS * ROWS, NOPE), 0)
    spread = [jnp.where(row16 % HEADS == h, nope_q, 0.0) for h in range(HEADS)]
    spread = jnp.concatenate(spread, axis=1).astype(BF16)
    loads[0].wait()
    lat_q = jnp.dot(spread, absorb[...], preferred_element_type=F32).astype(BF16)
    local_q[...] = lat_q.astype(F32)
    lat_q = local_q[...]
    qa[seq, :, :KVL] = lat_q[:ROWS].astype(BF16)
    qa[seq, :, KVL:] = rope_tile.astype(BF16)
    qb[seq] = lat_q[ROWS:].astype(BF16)

    pl.semaphore_wait(barrier, NZ - 1 + NY - 1)

    queries = (qa, qb)

    def settle(ref, sem):
        pltpu.make_async_copy(ref, ref, sem).wait()

    def gather_z(r, d):
        mine = queries[r].at[seq]
        return pltpu.make_async_remote_copy(
            src_ref=mine, dst_ref=mine, send_sem=agz_s.at[r], recv_sem=agz_r.at[r, min(d, NZ - d) - 1],
            device_id=at_z(d), device_id_type=pl.DeviceIdType.MESH)

    def gather_y(r, d, k):
        mine = queries[r].at[y * NZ + (z + k) % NZ]
        return pltpu.make_async_remote_copy(
            src_ref=mine, dst_ref=mine, send_sem=agy_s.at[r], recv_sem=agy_r.at[r, d - 1],
            device_id=at_y(d), device_id_type=pl.DeviceIdType.MESH)

    def pass_on(r, distance):
        senders = (distance,) if distance % (NZ // 2) == 0 else (distance, NZ - distance)
        if distance:
            settle(queries[r].at[pl.ds(0, len(senders))], agz_r.at[r, distance - 1])
        for d in senders:
            for e in FAR_Y:
                gather_y(r, e, (NZ - d) % NZ).start()

    def take_arrived(r, g):
        settle(queries[r].at[pl.ds(0, NZ)], agy_r.at[r, NY - GROUPS[g] - 1])
        take_group(r, g)

    def scatter_y(r, d):
        return pltpu.make_async_remote_copy(
            src_ref=partial.at[r, GROUPS.index(d)], dst_ref=yrecv.at[r, d - 1],
            send_sem=rsy_s.at[r], recv_sem=rsy_r.at[r],
            device_id=at_y(d), device_id_type=pl.DeviceIdType.MESH)

    def scatter_stats(r, d):
        return pltpu.make_async_remote_copy(
            src_ref=stats.at[r, GROUPS.index(d)], dst_ref=ystats.at[r, d - 1],
            send_sem=rst_s.at[r], recv_sem=rst_r.at[r],
            device_id=at_y(d), device_id_type=pl.DeviceIdType.MESH)

    def scatter_z(r, d):
        return pltpu.make_async_remote_copy(
            src_ref=zsend.at[r, (z + d) % NZ], dst_ref=zrecv.at[r, d - 1],
            send_sem=rsz_s.at[r], recv_sem=rsz_r.at[r],
            device_id=at_z(d), device_id_type=pl.DeviceIdType.MESH)

    for r in range(REQS):
        for d in NEAR_Z:
            gather_z(r, d).start()

    pass_on(0, 0)

    for copy in small_loads[2:]:
        copy.wait()
    freq = freq_ref[0:1]
    turn_sign = freq_ref[1:2]
    half_row = iota((ROPE, 128), 0)
    half_lane = iota((ROPE, 128), 1)
    new_latent = new_latent_ref[...].astype(F32)
    fresh = []
    lane_row = iota((8, 128), 0)
    positions = jnp.zeros((8, 128), jnp.int32)
    for r in range(REQS):
        for j in range(STEPS):
            positions = jnp.where(lane_row == r * STEPS + j, positions_ref[r, j], positions)
    angle = positions.astype(F32) * freq
    cosine, sine = jnp.cos(angle), jnp.sin(angle)
    row8n = iota((ROWS, 1), 0)
    for r in range(REQS):
        place = jnp.where(half_row + r * ROPE == half_lane, 1.0, 0.0).astype(BF16)
        swapped = jnp.where(
            (half_row + ROPE // 2) % ROPE + r * ROPE == half_lane, 1.0, 0.0).astype(BF16)
        plain = jnp.dot(new_rope_ref[...], place, preferred_element_type=F32)
        turned = jnp.dot(new_rope_ref[...], swapped, preferred_element_type=F32)
        found = []
        for j in range(STEPS):
            i = r * STEPS + j
            key = plain[i : i + 1] * cosine[i : i + 1] + turned[i : i + 1] * (sine[i : i + 1] * turn_sign)
            key = rounded(key)
            score = jnp.sum(lat_q[r * ROWS : (r + 1) * ROWS] * new_latent[r, j : j + 1], axis=1, keepdims=True)
            score = score + jnp.sum(rope_tile * key, axis=1, keepdims=True)
            found.append(jnp.where(row8n >= j * HEADS, score * SCORE_SCALE, MASKED))
        highest = functools.reduce(jnp.maximum, found)
        sums, totals = 0.0, 0.0
        for j in range(STEPS):
            weight = jnp.exp2(found[j] - highest)
            totals = totals + weight
            sums = sums + rounded(weight) * new_latent[r, j : j + 1]
        fresh.append((sums, highest, totals))

    lane128 = iota((GROUP, 128), 1)

    def take_group(r, g):
        rows = pl.ds(((y + GROUPS[g]) % NY) * NZ, NZ)
        at = pl.ds(g * GROUP, GROUP)
        qfull[r, at, :] = queries[r][rows, :, :KVL].astype(F32).reshape(GROUP, KVL).astype(BF16)
        turned = qa[rows, :, KVL:].astype(F32).reshape(GROUP, 128)
        rotary[r, at, :] = jnp.where(lane128 // ROPE == r, turned, 0.0).astype(BF16)

    def score(r, first, count):
        rows = pl.ds(first * GROUP, count * GROUP)
        query, turned = qfull[r, rows, :], rotary[r, rows, :]
        live = lengths_ref[r] - seq * KEYS
        peak = jnp.full((count * GROUP, 128), FLOOR, F32)
        for at in range(0, KEYS, SUB1):
            s = jnp.dot(query, flipped[r, :, at : at + SUB1], preferred_element_type=F32)
            s = s + jnp.dot(turned, keys[:, at : at + SUB1], preferred_element_type=F32)
            bias = jnp.where(at + iota((1, SUB1), 1) < live, 0.0, MASKED)
            s = s * SCORE_SCALE + bias
            scores[rows, at : at + SUB1] = s
            for t in range(SUB1 // 128):
                peak = jnp.maximum(peak, s[:, t * 128 : (t + 1) * 128])
        return jnp.max(peak, axis=1, keepdims=True)

    def weigh(r, first, count, highest):
        rows = pl.ds(first * GROUP, count * GROUP)
        lane_sums = jnp.zeros((count * GROUP, 128), F32)
        mixed = None
        for at in range(0, KEYS, SUB2):
            p = jnp.exp2(scores[rows, at : at + SUB2] - highest)
            for t in range(SUB2 // 128):
                lane_sums = lane_sums + p[:, t * 128 : (t + 1) * 128]
            piece = jnp.dot(p.astype(BF16), latent[r, at : at + SUB2, :], preferred_element_type=F32)
            mixed = piece if mixed is None else mixed + piece
        totals = jnp.sum(lane_sums, axis=1, keepdims=True)
        partial[r, pl.ds(first, count)] = mixed.reshape(count, NZ, ROWS, KVL).astype(BF16)
        for g in range(first, first + count):
            at = (g - first) * GROUP
            pair = jnp.where(lane128 == 0, highest[at : at + GROUP], totals[at : at + GROUP])
            stats[r, g] = pair.T[:8]
            if GROUPS[g]:
                scatter_y(r, GROUPS[g]).start()
                scatter_stats(r, GROUPS[g]).start()

    def flip(r, half):
        for at in range(half * KEYS // 2, (half + 1) * KEYS // 2, SUB1):
            flipped[r, :, at : at + SUB1] = latent[r, at : at + SUB1, :].T

    loads[1].wait()
    flip(0, 0)
    pass_on(0, 1)
    flip(0, 1)
    pass_on(0, 2)
    loads[2].wait()
    loads[3].wait()
    flip(1, 0)
    pass_on(0, 3)
    flip(1, 1)
    pass_on(0, 4)
    for distance in (0, 1, 2):
        pass_on(1, distance)
    take_group(0, 3)
    highest = score(0, 3, 1)
    for distance in (3, 4):
        pass_on(1, distance)
    weigh(0, 3, 1, highest)
    for g in (1, 2, 0):
        take_arrived(0, g)
    weigh(0, 0, 3, score(0, 0, 3))
    take_group(1, 3)
    for g in (1, 2, 0):
        take_arrived(1, g)
    highest = score(1, 0, 4)
    weigh(1, 0, 2, highest[: 2 * GROUP])
    weigh(1, 2, 2, highest[2 * GROUP :])

    for r in range(REQS):
        parts = [unpack_y(partial[r, GROUPS.index(0)], stats[r, GROUPS.index(0)])]
        settle(yrecv.at[r], rsy_r.at[r])
        settle(ystats.at[r], rst_r.at[r])
        for d in (1, 3, 2):
            parts.append(unpack_y(yrecv[r, d - 1], ystats[r, d - 1]))
        sums, highest, totals = merge(parts)
        zsend[r, :, :, :KVL] = sums.reshape(NZ, ROWS, KVL).astype(BF16)
        zsend[r, :, :, KVL:] = encode(highest, totals).reshape(NZ, ROWS, 128).astype(BF16)
        for d in FAR_Z:
            scatter_z(r, d).start()

    loads[4].wait()
    results = []
    for r in range(REQS):
        parts = [fresh[r], unpack(zsend[r, z].astype(F32))]
        settle(zrecv.at[r], rsz_r.at[r])
        for d in FAR_Z[::-1]:
            parts.append(unpack(zrecv[r, d - 1].astype(F32)))
        sums, highest, totals = merge(parts)
        results.append(rounded(sums / totals))
    result = jnp.concatenate(results, axis=0)
    row16v = iota((REQS * ROWS, KVL), 0)
    spread = [jnp.where(row16v % HEADS == h, result, 0.0) for h in range(HEADS)]
    spread = jnp.concatenate(spread, axis=1).astype(BF16)
    out_ref[...] = jnp.dot(spread, value[...], preferred_element_type=F32).astype(BF16)

    for r in range(REQS):
        settle(queries[r].at[pl.ds(0, NZ - 1)], agz_s.at[r])
        settle(queries[r].at[pl.ds(0, (NY - 1) * NZ)], agy_s.at[r])
        settle(partial.at[r, pl.ds(0, NY - 1)], rsy_s.at[r])
        settle(stats.at[r, pl.ds(0, NY - 1)], rst_s.at[r])
        settle(zsend.at[r, pl.ds(0, NZ - 1)], rsz_s.at[r])


def frequency_rows():
    half = ROPE // 2
    lanes = np.arange(128)
    freq = (10000.0 ** (-(np.arange(half, dtype=np.float64)) / half)).astype(np.float32)
    sign = np.where(lanes % ROPE < half, -1.0, 1.0).astype(np.float32)
    return np.stack([freq[lanes % half], sign])


def on_device(
    query_nope, query_rope, key_absorb, value_up_matrix, latent_cache, rope_cache,
    new_latent, new_rope, lengths, positions,
):
    vmem = pl.BlockSpec(memory_space=pltpu.VMEM)
    hbm = pl.BlockSpec(memory_space=pltpu.HBM)
    pin = lambda x: pltpu.with_memory_space_constraint(x, pltpu.HBM)
    out = pl.pallas_call(
        kernel,
        name="latent_attention",
        out_shape=jax.ShapeDtypeStruct((REQS * ROWS, VH), BF16),
        in_specs=[hbm] * 11,
        out_specs=vmem,
        scratch_shapes=[
            pltpu.VMEM((REQS * ROWS, NOPE), BF16),
            pltpu.VMEM((REQS, STEPS, HEADS * ROPE), BF16),
            pltpu.VMEM((REQS, STEPS, KVL), BF16),
            pltpu.VMEM((REQS * STEPS, ROPE), BF16),
            pltpu.VMEM((2, 128), F32),
            pltpu.SMEM((REQS,), jnp.int32),
            pltpu.SMEM((REQS, STEPS), jnp.int32),
            pltpu.VMEM((HEADS * NOPE, KVL), BF16),
            pltpu.VMEM((HEADS * KVL, VH), BF16),
            pltpu.VMEM((REQS, KEYS, KVL), BF16),
            pltpu.VMEM((REQS * ROPE, KEYS), BF16),
            pltpu.VMEM((SHARDS, ROWS, WIDE), BF16),
            pltpu.VMEM((SHARDS, ROWS, KVL), BF16),
            pltpu.VMEM((REQS, ALL, KVL), BF16),
            pltpu.VMEM((REQS, ALL, 128), BF16),
            pltpu.VMEM((REQS, KVL, KEYS), BF16),
            pltpu.VMEM((ALL, KEYS), F32),
            pltpu.VMEM((REQS * ROWS, KVL), F32),
            pltpu.VMEM((REQS, NY, NZ, ROWS, KVL), BF16),
            pltpu.VMEM((REQS, NY, 8, GROUP), F32),
            pltpu.VMEM((REQS, NY - 1, NZ, ROWS, KVL), BF16),
            pltpu.VMEM((REQS, NY - 1, 8, GROUP), F32),
            pltpu.VMEM((REQS, NZ, ROWS, WIDE), BF16),
            pltpu.VMEM((REQS, NZ - 1, ROWS, WIDE), BF16),
            pltpu.SemaphoreType.DMA((7,)),
            pltpu.SemaphoreType.DMA((5,)),
            pltpu.SemaphoreType.DMA((REQS,)),
            pltpu.SemaphoreType.DMA((REQS, NZ // 2)),
            pltpu.SemaphoreType.DMA((REQS,)),
            pltpu.SemaphoreType.DMA((REQS, NY - 1)),
            pltpu.SemaphoreType.DMA((REQS,)),
            pltpu.SemaphoreType.DMA((REQS,)),
            pltpu.SemaphoreType.DMA((REQS,)),
            pltpu.SemaphoreType.DMA((REQS,)),
            pltpu.SemaphoreType.DMA((REQS,)),
            pltpu.SemaphoreType.DMA((REQS,)),
        ],
        compiler_params=pltpu.CompilerParams(collective_id=0, has_side_effects=True, vmem_limit_bytes=VMEM_LIMIT),
    )(*map(pin, (
        query_nope.reshape(REQS * ROWS, NOPE),
        query_rope,
        key_absorb.reshape(HEADS * NOPE, KVL),
        value_up_matrix.reshape(HEADS * KVL, VH),
        latent_cache,
        rope_cache.reshape(REQS * ROPE, KEYS),
        new_latent,
        new_rope.reshape(REQS * STEPS, ROPE),
        jnp.asarray(frequency_rows()),
        lengths,
        positions,
    )))
    return out.reshape(REQS, STEPS, HEADS, VH)


def solution(mesh):
    return jax.shard_map(
        on_device,
        mesh=mesh,
        in_specs=(
            P("req", None, "seq", None),
            P("req", None, "seq"),
            P("seq", None, None),
            P("seq", None, None),
            P("req", "seq", None),
            P("req", None, "seq"),
            P("req", None, None),
            P("req", None, None),
            P("req"),
            P("req", None),
        ),
        out_specs=P("req", None, "seq", None),
        check_vma=False,
    )
```

```python
import functools

import jax
import jax.numpy as jnp
import numpy as np
from jax import lax
from jax.experimental import pallas as pl
from jax.experimental.pallas import tpu as pltpu
from jax.sharding import PartitionSpec as P

F32 = jnp.float32
BF16 = jnp.bfloat16
MASKED = -1e30
FLOOR = -1e29
NY, NZ = 4, 8
SHARDS = NY * NZ
REQS, STEPS, HEADS, NOPE, KVL, ROPE, VH = 2, 2, 4, 128, 512, 64, 128
ROWS = STEPS * HEADS
ALL = SHARDS * ROWS
KEYS = 4096
WIDE = KVL + 128
SCORE_SCALE = float((NOPE + ROPE) ** -0.5 * np.log2(np.e))
SUB1 = 512
SUB2 = 256
FAR_Z = (4, 3, 5, 2, 6, 1, 7)
ORDER_Z = FAR_Z + (0,)
FAR = 3
SPANS = (pl.ds(0, FAR), pl.ds(FAR, NZ - FAR))
NEAR_Z = (1, 7, 2, 6, 3, 5, 4)
FAR_Y = (1, 3, 2)
VMEM_LIMIT = 40 << 20
GROUPS = (2, 1, 3, 0)
GROUP = NZ * ROWS


def iota(shape, dim):
    return lax.broadcasted_iota(jnp.int32, shape, dim)


def rounded(x):
    return x.astype(BF16).astype(F32)


def encode(maxima, totals):
    rows = maxima.shape[0]
    lane = iota((rows, 128), 1)
    high = rounded(maxima)
    middle = rounded(maxima - high)
    low = maxima - high - middle
    total_high = rounded(totals)
    total_low = totals - total_high
    tile = jnp.where(lane == 0, high, 0.0)
    tile = jnp.where(lane == 1, middle, tile)
    tile = jnp.where(lane == 2, low, tile)
    tile = jnp.where(lane == 3, total_high, tile)
    return jnp.where(lane == 4, total_low, tile)


def decode(tile):
    lane = iota(tile.shape, 1)
    maxima = jnp.sum(jnp.where(lane < 3, tile, 0.0), axis=1, keepdims=True)
    totals = jnp.sum(jnp.where(lane < 3, 0.0, tile), axis=1, keepdims=True)
    return maxima, totals


def merge(parts):
    highest = functools.reduce(jnp.maximum, [m for _, m, _ in parts])
    sums, totals = 0.0, 0.0
    for s, m, t in parts:
        factor = jnp.exp2(m - highest)
        sums = sums + s * factor
        totals = totals + t * factor
    return sums, highest, totals


def unpack(block):
    wide = block.astype(F32)
    return (wide[:, :KVL],) + decode(wide[:, KVL:])


def kernel(
    nope_hbm, rope_hbm, absorb_hbm, value_hbm, latent_hbm, keys_hbm,
    new_latent_hbm, new_rope_hbm, freq_hbm, lengths_hbm, positions_hbm,
    out_ref,
    nope_ref, rope_ref, new_latent_ref, new_rope_ref, freq_ref, lengths_ref, positions_ref,
    absorb, value, latent, keys, qa, qb, qfull, rotary, flipped, scores, local_q,
    partial, stats, yfar, ynear, ystats, zsend, zrecv,
    small_sem, load_sem, agz_s, agz_r, agy_s, agy_r, rsy_s, rsy_r, rst_s, rst_r, rsz_s, rsz_r,
):
    seq = lax.axis_index("seq")
    y = seq // NZ
    z = seq % NZ

    def at_z(d):
        return {"seq": y * NZ + (z + d) % NZ}

    def at_y(d):
        return {"seq": ((y + d) % NY) * NZ + z}

    barrier = pltpu.get_barrier_semaphore()
    for d in FAR_Z:
        pl.semaphore_signal(barrier, inc=1, device_id=at_z(d), device_id_type=pl.DeviceIdType.MESH)
    for d in FAR_Y:
        pl.semaphore_signal(barrier, inc=1, device_id=at_y(d), device_id_type=pl.DeviceIdType.MESH)

    small = (
        (nope_hbm, nope_ref), (rope_hbm, rope_ref), (new_latent_hbm, new_latent_ref),
        (new_rope_hbm, new_rope_ref), (freq_hbm, freq_ref), (lengths_hbm, lengths_ref),
        (positions_hbm, positions_ref),
    )
    small_loads = [pltpu.make_async_copy(a, b, small_sem.at[i]) for i, (a, b) in enumerate(small)]
    for copy in small_loads:
        copy.start()
    loads = [
        pltpu.make_async_copy(absorb_hbm, absorb, load_sem.at[0]),
        pltpu.make_async_copy(latent_hbm.at[0], latent.at[0], load_sem.at[1]),
        pltpu.make_async_copy(keys_hbm, keys, load_sem.at[2]),
        pltpu.make_async_copy(latent_hbm.at[1], latent.at[1], load_sem.at[3]),
        pltpu.make_async_copy(value_hbm, value, load_sem.at[4]),
    ]
    for copy in loads:
        copy.start()

    small_loads[1].wait()
    rope_q = rope_ref[...].astype(F32)
    row8 = iota((ROWS, HEADS * ROPE), 0)
    lane256 = iota((ROWS, HEADS * ROPE), 1)
    fold_row = iota((HEADS * ROPE, 128), 0)
    fold_lane = iota((HEADS * ROPE, 128), 1)
    rope_tile = jnp.zeros((ROWS, 128), F32)
    for r in range(REQS):
        spread = jnp.where(row8 < HEADS, rope_q[r, 0:1], rope_q[r, 1:2])
        spread = jnp.where(lane256 // ROPE == row8 % HEADS, spread, 0.0).astype(BF16)
        fold = jnp.where(fold_row % ROPE + r * ROPE == fold_lane, 1.0, 0.0).astype(BF16)
        rope_tile = rope_tile + jnp.dot(spread, fold, preferred_element_type=F32)
    small_loads[0].wait()
    nope_q = nope_ref[...].astype(F32)
    row16 = iota((REQS * ROWS, NOPE), 0)
    spread = [jnp.where(row16 % HEADS == h, nope_q, 0.0) for h in range(HEADS)]
    spread = jnp.concatenate(spread, axis=1).astype(BF16)
    loads[0].wait()
    lat_q = jnp.dot(spread, absorb[...], preferred_element_type=F32).astype(BF16)
    local_q[...] = lat_q.astype(F32)
    lat_q = local_q[...]
    qa[seq, :, :KVL] = lat_q[:ROWS].astype(BF16)
    qa[seq, :, KVL:] = rope_tile.astype(BF16)
    qb[seq] = lat_q[ROWS:].astype(BF16)

    pl.semaphore_wait(barrier, NZ - 1 + NY - 1)

    queries = (qa, qb)
    yrecv = (yfar, ynear)

    def settle(ref, sem):
        pltpu.make_async_copy(ref, ref, sem).wait()

    def gather_z(r, d):
        mine = queries[r].at[seq]
        return pltpu.make_async_remote_copy(
            src_ref=mine, dst_ref=mine, send_sem=agz_s.at[r], recv_sem=agz_r.at[r, min(d, NZ - d) - 1],
            device_id=at_z(d), device_id_type=pl.DeviceIdType.MESH)

    def gather_y(r, d, k):
        mine = queries[r].at[y * NZ + (z + k) % NZ]
        return pltpu.make_async_remote_copy(
            src_ref=mine, dst_ref=mine, send_sem=agy_s.at[r], recv_sem=agy_r.at[r, d - 1],
            device_id=at_y(d), device_id_type=pl.DeviceIdType.MESH)

    def pass_on(r, distance):
        senders = (distance,) if distance % (NZ // 2) == 0 else (distance, NZ - distance)
        if distance:
            settle(queries[r].at[pl.ds(0, len(senders))], agz_r.at[r, distance - 1])
        for d in senders:
            for e in FAR_Y:
                gather_y(r, e, (NZ - d) % NZ).start()

    def take_arrived(r, g):
        settle(queries[r].at[pl.ds(0, NZ)], agy_r.at[r, NY - GROUPS[g] - 1])
        take_group(r, g)

    def scatter_y(r, d, part):
        return pltpu.make_async_remote_copy(
            src_ref=partial.at[r, GROUPS.index(d), SPANS[part]], dst_ref=yrecv[part].at[r, d - 1],
            send_sem=rsy_s.at[r], recv_sem=rsy_r.at[r, part],
            device_id=at_y(d), device_id_type=pl.DeviceIdType.MESH)

    def scatter_stats(r, d):
        return pltpu.make_async_remote_copy(
            src_ref=stats.at[r, GROUPS.index(d)], dst_ref=ystats.at[r, d - 1],
            send_sem=rst_s.at[r], recv_sem=rst_r.at[r],
            device_id=at_y(d), device_id_type=pl.DeviceIdType.MESH)

    def scatter_z(r, d):
        return pltpu.make_async_remote_copy(
            src_ref=zsend.at[r, ORDER_Z.index(d)], dst_ref=zrecv.at[r, d - 1],
            send_sem=rsz_s.at[r], recv_sem=rsz_r.at[r],
            device_id=at_z(d), device_id_type=pl.DeviceIdType.MESH)

    for d in NEAR_Z:
        gather_z(0, d).start()

    pass_on(0, 0)

    for copy in small_loads[2:]:
        copy.wait()
    freq = freq_ref[0:1]
    turn_sign = freq_ref[1:2]
    half_row = iota((ROPE, 128), 0)
    half_lane = iota((ROPE, 128), 1)
    new_latent = new_latent_ref[...].astype(F32)
    fresh = []
    lane_row = iota((8, 128), 0)
    positions = jnp.zeros((8, 128), jnp.int32)
    for r in range(REQS):
        for j in range(STEPS):
            positions = jnp.where(lane_row == r * STEPS + j, positions_ref[r, j], positions)
    angle = positions.astype(F32) * freq
    cosine, sine = jnp.cos(angle), jnp.sin(angle)
    row8n = iota((ROWS, 1), 0)
    for r in range(REQS):
        place = jnp.where(half_row + r * ROPE == half_lane, 1.0, 0.0).astype(BF16)
        swapped = jnp.where(
            (half_row + ROPE // 2) % ROPE + r * ROPE == half_lane, 1.0, 0.0).astype(BF16)
        plain = jnp.dot(new_rope_ref[...], place, preferred_element_type=F32)
        turned = jnp.dot(new_rope_ref[...], swapped, preferred_element_type=F32)
        found = []
        for j in range(STEPS):
            i = r * STEPS + j
            key = plain[i : i + 1] * cosine[i : i + 1] + turned[i : i + 1] * (sine[i : i + 1] * turn_sign)
            key = rounded(key)
            score = jnp.sum(lat_q[r * ROWS : (r + 1) * ROWS] * new_latent[r, j : j + 1], axis=1, keepdims=True)
            score = score + jnp.sum(rope_tile * key, axis=1, keepdims=True)
            found.append(jnp.where(row8n >= j * HEADS, score * SCORE_SCALE, MASKED))
        highest = functools.reduce(jnp.maximum, found)
        sums, totals = 0.0, 0.0
        for j in range(STEPS):
            weight = jnp.exp2(found[j] - highest)
            totals = totals + weight
            sums = sums + rounded(weight) * new_latent[r, j : j + 1]
        fresh.append((sums, highest, totals))

    lane128 = iota((GROUP, 128), 1)

    def take_group(r, g):
        line = ((y + GROUPS[g]) % NY) * NZ
        at = pl.ds(g * GROUP, GROUP)
        blocks = [line + (z + d) % NZ for d in ORDER_Z]
        rows = [queries[r][i, :, :KVL].astype(F32) for i in blocks]
        qfull[r, at, :] = jnp.concatenate(rows, axis=0).astype(BF16)
        turned = jnp.concatenate([qa[i, :, KVL:].astype(F32) for i in blocks], axis=0)
        rotary[r, at, :] = jnp.where(lane128 // ROPE == r, turned, 0.0).astype(BF16)

    def score(r, first, count):
        rows = pl.ds(first * GROUP, count * GROUP)
        query, turned = qfull[r, rows, :], rotary[r, rows, :]
        live = lengths_ref[r] - seq * KEYS
        peak = jnp.full((count * GROUP, 128), FLOOR, F32)
        for at in range(0, KEYS, SUB1):
            s = jnp.dot(query, flipped[r, :, at : at + SUB1], preferred_element_type=F32)
            s = s + jnp.dot(turned, keys[:, at : at + SUB1], preferred_element_type=F32)
            bias = jnp.where(at + iota((1, SUB1), 1) < live, 0.0, MASKED)
            s = s * SCORE_SCALE + bias
            scores[r, rows, at : at + SUB1] = s
            for t in range(SUB1 // 128):
                peak = jnp.maximum(peak, s[:, t * 128 : (t + 1) * 128])
        return jnp.max(peak, axis=1, keepdims=True)

    def weigh(r, first, count, highest):
        rows = pl.ds(first * GROUP, count * GROUP)
        lane_sums = jnp.zeros((count * GROUP, 128), F32)
        mixed = None
        for at in range(0, KEYS, SUB2):
            p = jnp.exp2(scores[r, rows, at : at + SUB2] - highest)
            for t in range(SUB2 // 128):
                lane_sums = lane_sums + p[:, t * 128 : (t + 1) * 128]
            piece = jnp.dot(p.astype(BF16), latent[r, at : at + SUB2, :], preferred_element_type=F32)
            mixed = piece if mixed is None else mixed + piece
        totals = jnp.sum(lane_sums, axis=1, keepdims=True)
        partial[r, pl.ds(first, count)] = mixed.reshape(count, NZ, ROWS, KVL).astype(BF16)
        for g in range(first, first + count):
            at = (g - first) * GROUP
            pair = jnp.where(lane128 == 0, highest[at : at + GROUP], totals[at : at + GROUP])
            stats[r, g] = pair.T[:8]
        away = [d for d in GROUPS[first : first + count] if d]
        for d in away:
            scatter_stats(r, d).start()
        for part in range(2):
            for d in away:
                scatter_y(r, d, part).start()

    def flip(r, half):
        for at in range(half * KEYS // 2, (half + 1) * KEYS // 2, SUB1):
            flipped[r, :, at : at + SUB1] = latent[r, at : at + SUB1, :].T

    loads[1].wait()
    flip(0, 0)
    pass_on(0, 1)
    for d in NEAR_Z:
        gather_z(1, d).start()
    flip(0, 1)
    pass_on(0, 2)
    loads[2].wait()
    loads[3].wait()
    flip(1, 0)
    pass_on(0, 3)
    flip(1, 1)
    pass_on(0, 4)
    take_group(0, 3)
    own = [score(0, 3, 1)]
    for distance in (0, 1, 2):
        pass_on(1, distance)
    for distance in (3, 4):
        pass_on(1, distance)
    take_group(1, 3)
    own.append(score(1, 3, 1))
    for r in range(REQS):
        for g in (1, 2, 0):
            take_arrived(r, g)
        highest = score(r, 0, 3)
        weigh(r, 0, 2, highest[: 2 * GROUP])
        weigh(r, 2, 2, jnp.concatenate([highest[2 * GROUP :], own[r]], axis=0))

    for r in range(REQS):
        for part in range(2):
            first, count = (0, FAR) if part == 0 else (FAR, NZ - FAR)
            settle(yrecv[part].at[r], rsy_r.at[r, part])
            if part == 0:
                settle(ystats.at[r], rst_r.at[r])
                columns = [stats[r, GROUPS.index(0)].T] + [ystats[r, d - 1].T for d in (1, 3, 2)]
            blocks = [partial[r, GROUPS.index(0), SPANS[part]]]
            blocks = blocks + [yrecv[part][r, d - 1] for d in (1, 3, 2)]
            parts = []
            for block, column in zip(blocks, columns):
                column = column[first * ROWS : (first + count) * ROWS]
                block = block.astype(F32).reshape(count * ROWS, KVL)
                parts.append((block, column[:, 0:1], column[:, 1:2]))
            sums, highest, totals = merge(parts)
            tile = encode(highest, totals)
            zsend[r, SPANS[part], :, :KVL] = sums.reshape(count, ROWS, KVL).astype(BF16)
            zsend[r, SPANS[part], :, KVL:] = tile.reshape(count, ROWS, 128).astype(BF16)
            for d in ORDER_Z[first : first + count]:
                if d:
                    scatter_z(r, d).start()

    loads[4].wait()
    results = []
    for r in range(REQS):
        parts = [fresh[r], unpack(zsend[r, ORDER_Z.index(0)].astype(F32))]
        settle(zrecv.at[r], rsz_r.at[r])
        for d in FAR_Z[::-1]:
            parts.append(unpack(zrecv[r, d - 1].astype(F32)))
        sums, highest, totals = merge(parts)
        results.append(rounded(sums / totals))
    result = jnp.concatenate(results, axis=0)
    row16v = iota((REQS * ROWS, KVL), 0)
    spread = [jnp.where(row16v % HEADS == h, result, 0.0) for h in range(HEADS)]
    spread = jnp.concatenate(spread, axis=1).astype(BF16)
    out_ref[...] = jnp.dot(spread, value[...], preferred_element_type=F32).astype(BF16)

    for r in range(REQS):
        settle(queries[r].at[pl.ds(0, NZ - 1)], agz_s.at[r])
        settle(queries[r].at[pl.ds(0, (NY - 1) * NZ)], agy_s.at[r])
        settle(partial.at[r, pl.ds(0, NY - 1)], rsy_s.at[r])
        settle(stats.at[r, pl.ds(0, NY - 1)], rst_s.at[r])
        settle(zsend.at[r, pl.ds(0, NZ - 1)], rsz_s.at[r])


def frequency_rows():
    half = ROPE // 2
    lanes = np.arange(128)
    freq = (10000.0 ** (-(np.arange(half, dtype=np.float64)) / half)).astype(np.float32)
    sign = np.where(lanes % ROPE < half, -1.0, 1.0).astype(np.float32)
    return np.stack([freq[lanes % half], sign])


def on_device(
    query_nope, query_rope, key_absorb, value_up_matrix, latent_cache, rope_cache,
    new_latent, new_rope, lengths, positions,
):
    vmem = pl.BlockSpec(memory_space=pltpu.VMEM)
    hbm = pl.BlockSpec(memory_space=pltpu.HBM)
    pin = lambda x: pltpu.with_memory_space_constraint(x, pltpu.HBM)
    out = pl.pallas_call(
        kernel,
        name="latent_attention",
        out_shape=jax.ShapeDtypeStruct((REQS * ROWS, VH), BF16),
        in_specs=[hbm] * 11,
        out_specs=vmem,
        scratch_shapes=[
            pltpu.VMEM((REQS * ROWS, NOPE), BF16),
            pltpu.VMEM((REQS, STEPS, HEADS * ROPE), BF16),
            pltpu.VMEM((REQS, STEPS, KVL), BF16),
            pltpu.VMEM((REQS * STEPS, ROPE), BF16),
            pltpu.VMEM((2, 128), F32),
            pltpu.SMEM((REQS,), jnp.int32),
            pltpu.SMEM((REQS, STEPS), jnp.int32),
            pltpu.VMEM((HEADS * NOPE, KVL), BF16),
            pltpu.VMEM((HEADS * KVL, VH), BF16),
            pltpu.VMEM((REQS, KEYS, KVL), BF16),
            pltpu.VMEM((REQS * ROPE, KEYS), BF16),
            pltpu.VMEM((SHARDS, ROWS, WIDE), BF16),
            pltpu.VMEM((SHARDS, ROWS, KVL), BF16),
            pltpu.VMEM((REQS, ALL, KVL), BF16),
            pltpu.VMEM((REQS, ALL, 128), BF16),
            pltpu.VMEM((REQS, KVL, KEYS), BF16),
            pltpu.VMEM((REQS, ALL, KEYS), F32),
            pltpu.VMEM((REQS * ROWS, KVL), F32),
            pltpu.VMEM((REQS, NY, NZ, ROWS, KVL), BF16),
            pltpu.VMEM((REQS, NY, 8, GROUP), F32),
            pltpu.VMEM((REQS, NY - 1, FAR, ROWS, KVL), BF16),
            pltpu.VMEM((REQS, NY - 1, NZ - FAR, ROWS, KVL), BF16),
            pltpu.VMEM((REQS, NY - 1, 8, GROUP), F32),
            pltpu.VMEM((REQS, NZ, ROWS, WIDE), BF16),
            pltpu.VMEM((REQS, NZ - 1, ROWS, WIDE), BF16),
            pltpu.SemaphoreType.DMA((7,)),
            pltpu.SemaphoreType.DMA((5,)),
            pltpu.SemaphoreType.DMA((REQS,)),
            pltpu.SemaphoreType.DMA((REQS, NZ // 2)),
            pltpu.SemaphoreType.DMA((REQS,)),
            pltpu.SemaphoreType.DMA((REQS, NY - 1)),
            pltpu.SemaphoreType.DMA((REQS,)),
            pltpu.SemaphoreType.DMA((REQS, 2)),
            pltpu.SemaphoreType.DMA((REQS,)),
            pltpu.SemaphoreType.DMA((REQS,)),
            pltpu.SemaphoreType.DMA((REQS,)),
            pltpu.SemaphoreType.DMA((REQS,)),
        ],
        compiler_params=pltpu.CompilerParams(collective_id=0, has_side_effects=True, vmem_limit_bytes=VMEM_LIMIT),
    )(*map(pin, (
        query_nope.reshape(REQS * ROWS, NOPE),
        query_rope,
        key_absorb.reshape(HEADS * NOPE, KVL),
        value_up_matrix.reshape(HEADS * KVL, VH),
        latent_cache,
        rope_cache.reshape(REQS * ROPE, KEYS),
        new_latent,
        new_rope.reshape(REQS * STEPS, ROPE),
        jnp.asarray(frequency_rows()),
        lengths,
        positions,
    )))
    return out.reshape(REQS, STEPS, HEADS, VH)


def solution(mesh):
    return jax.shard_map(
        on_device,
        mesh=mesh,
        in_specs=(
            P("req", None, "seq", None),
            P("req", None, "seq"),
            P("seq", None, None),
            P("seq", None, None),
            P("req", "seq", None),
            P("req", None, "seq"),
            P("req", None, None),
            P("req", None, None),
            P("req"),
            P("req", None),
        ),
        out_specs=P("req", None, "seq", None),
        check_vma=False,
    )
```
